1024 devices in a mesh: gx: 64 (over x, z), gy: 16 (over y, core).
Axes of the slice: x: 8, y: 8, z: 8, core: 2. Of those that a mesh axis runs over, the one named last changes fastest.
Arguments:
- species: float32 [53, 256, 128, 128], P(None, 'gx', 'gy'), may hold values from -6 to 6
- diffusion: float32 [53], replicated, may hold values from 0.02 to 0.15
- class_rate: float32 [4], replicated, may hold values from 0.2 to 1
- mixing: float32 [53, 53], replicated, may hold values from -0.3 to 0.3
- inverses: float32 [4, 53, 53], replicated, may hold values from -0.01 to 0.12
- newton_counts: int32 [4], replicated, may hold values from 1 to 8, as said below
- cell_class: int32 [256, 128, 128], P('gx', 'gy'), may hold values from 0 to 3
Outputs:
- updated: float32 [53, 256, 128, 128], P(None, 'gx', 'gy')
The draws below stay inside these ranges and needn't reach their ends.
Inputs may be any that keep to these rules, and one draw needn't show every extreme that they name: `newton_counts`: nondecreasing in the class; the last class takes 8.
All inputs are finite; a program needn't handle non-finite values.
Results may differ from the reference program's by a relative error of at most 0.0003.
Values sent between devices are 32-bit elements; how exact they have to be, the bound alone decides.
A program may use at most 32 MiB of HBM per device.

```python
import math
import jax
import jax.numpy as jnp
from jax import lax

SPEC = 53
NCLASS = 4
NMAX = 8
NZ = 128
NX = 256
NY = 128


def draw_inverses(key, part):
    first, second = jax.random.split(jax.random.fold_in(key, 5))
    diag = jnp.exp(jax.random.uniform(first, (NCLASS, SPEC), jnp.float32, math.log(0.06), math.log(0.12)))
    spread = jax.random.normal(second, (NCLASS, SPEC, SPEC), jnp.float32)
    spread = jnp.clip(spread * (0.0225 / math.sqrt(SPEC)), -0.01, 0.01)
    identity = jnp.eye(SPEC, dtype=jnp.float32)[None]
    return spread * (1.0 - identity) + diag[:, :, None] * identity


def draw_newton_counts(key, part):
    base = jax.random.randint(jax.random.fold_in(key, 11), (NCLASS,), 1, NMAX + 1)
    base = jnp.sort(base)
    return base.at[NCLASS - 1].set(NMAX).astype(jnp.int32)


def draw_cell_class(key, part):
    front_key, heavy_key, pick_key, light_key = jax.random.split(jax.random.fold_in(key, 23), 4)
    front = jax.random.randint(front_key, (), 0, NX)
    positions = jnp.arange(NX, dtype=jnp.int32)[:, None, None]
    near = jnp.abs(positions - front) < max(NX // 16, 1)
    shape = (NX, NY, NZ)
    heavy = jax.random.randint(heavy_key, shape, 1, NCLASS)
    picked = jax.random.randint(pick_key, shape, 0, 8)
    light = jnp.where(picked == 0, jax.random.randint(light_key, shape, 0, NCLASS), 0)
    return jnp.where(near, heavy, light).astype(jnp.int32)


def level_of(stream_key, shape, shards, least, largest):
    gain = 1.0
    for dim, shards_of in shards:
        draws = jax.random.uniform(jax.random.fold_in(jax.random.fold_in(stream_key, 6), dim), (shards_of,), jnp.float32, least / len(shards), largest / len(shards))
        gain = gain * jnp.repeat(jnp.exp(draws), shape[dim] // shards_of).reshape((-1,) + (1,) * (len(shape) - 1 - dim))
    return gain


def normal_values(own_key, extent, scale, bound, cuts=(), held_as=jnp.bfloat16):
    level = level_of(own_key, extent, cuts, -0.22, 0.18) if cuts else 1.0
    values = jax.random.normal(own_key, extent, jnp.float32) * scale * level
    return jnp.minimum(jnp.maximum(values, -bound), bound).astype(held_as)


def setup_inputs(seed: int = 0) -> dict:
    arg_keys = jax.random.split(jax.random.key(seed), 8)
    species = normal_values(arg_keys[0], (SPEC, NX, NY, NZ), 1.0, 6.0, ((1, 64), (2, 16)), jnp.float32)
    diffusion = jnp.clip(jnp.exp(jax.random.uniform(arg_keys[1], (SPEC,), jnp.float32, math.log(0.02), math.log(0.15))), 0.02, 0.15)
    class_rate = jnp.clip(jnp.exp(jax.random.uniform(arg_keys[2], (NCLASS,), jnp.float32, math.log(0.2), math.log(1.0))), 0.2, 1.0)
    mixing = normal_values(arg_keys[3], (SPEC, SPEC), (0.3 * SPEC ** -0.5), 0.3, (), jnp.float32)
    inverses = draw_inverses(jax.random.fold_in(arg_keys[7], 71), 0)
    newton_counts = draw_newton_counts(jax.random.fold_in(arg_keys[7], 71), 0)
    cell_class = draw_cell_class(jax.random.fold_in(arg_keys[7], 71), 0)
    return {"species": species, "diffusion": diffusion, "class_rate": class_rate, "mixing": mixing, "inverses": inverses, "newton_counts": newton_counts, "cell_class": cell_class}


def laplace(grid_field):
    padded = jnp.pad(grid_field, 1)
    total = padded[2:, 1:-1, 1:-1] + padded[:-2, 1:-1, 1:-1]
    total = total + padded[1:-1, 2:, 1:-1] + padded[1:-1, :-2, 1:-1]
    total = total + padded[1:-1, 1:-1, 2:] + padded[1:-1, 1:-1, :-2]
    return total - 6.0 * grid_field


def newton_cells(target, classes, class_rate, mixing, inverses, newton_counts):
    class_mask = (classes[None, :] == jnp.arange(NCLASS, dtype=jnp.int32)[:, None])
    weights = class_mask.astype(jnp.float32)
    cell_rate = jnp.sum(class_rate[:, None] * weights, axis=0)
    cell_count = jnp.sum(jnp.where(class_mask, newton_counts[:, None], 0), axis=0)

    def newton_step(k, state):
        source = jnp.dot(mixing, jnp.tanh(state), precision=lax.Precision.HIGHEST) - state
        residual = state - target - cell_rate * source
        correction = jnp.zeros_like(state)
        for which in range(NCLASS):
            correction = correction + weights[which] * jnp.dot(inverses[which], residual, precision=lax.Precision.HIGHEST)
        return jnp.where(k < cell_count, state - correction, state)

    return lax.fori_loop(0, NMAX, newton_step, target)


def reference(species, diffusion, class_rate, mixing, inverses, newton_counts, cell_class):
    forcing = lax.map(laplace, species) * diffusion[:, None, None, None]
    target = species + forcing
    moved = jnp.moveaxis(target, 1, 0)

    def solve_slice(pair):
        slab, slab_class = pair
        solved = newton_cells(slab.reshape(SPEC, -1), slab_class.reshape(-1), class_rate, mixing, inverses, newton_counts)
        return solved.reshape(slab.shape)

    section_value = jnp.moveaxis(lax.map(solve_slice, (moved, cell_class)), 0, 1)
    second = lax.map(laplace, section_value) * diffusion[:, None, None, None]
    return section_value + 0.5 * (second - forcing)
```

```python
import functools

import jax
import jax.numpy as jnp
from jax import lax
from jax.experimental import pallas as pl
from jax.experimental.pallas import tpu as pltpu
from jax.sharding import PartitionSpec as P

SPEC = 53
PAD = 56
NCLASS = 4
NMAX = 8
F32, BF16 = jnp.float32, jnp.bfloat16
MESH = pl.DeviceIdType.MESH

MIX_LAG = 4
INV_LAG = 8
UNROLL = 4


def split3(v):
    v = jnp.concatenate([v, jnp.zeros((8, v.shape[1]), F32)], axis=0)
    high = v.astype(BF16)
    low = (v - high.astype(F32)).astype(BF16)
    return jnp.concatenate([high, low, high], axis=0)


def weight_split(w):
    high = w.astype(BF16).astype(F32)
    low = w - high
    both = high + pltpu.roll(high, 64, 1)
    return jnp.concatenate([both.astype(BF16), low.astype(BF16)], axis=1)


def newton(units, state, scaled, ratio, classes, wmix, winv):
    count = len(units)

    def body(trip, carry):
        mixed, moved = {}, {}
        steps = count * UNROLL
        for i in range(steps + INV_LAG):
            j = i - INV_LAG
            if 0 <= j < steps:
                out = moved.pop(j)
                for lane, (x, y) in enumerate(units[j % count]):
                    which = jnp.broadcast_to(classes[x, y : y + 1, :], (PAD, 128))
                    part = out[:, lane * 128 : (lane + 1) * 128]
                    correction = jnp.where(
                        which == 0,
                        part[0:PAD],
                        jnp.where(
                            which == 1,
                            part[PAD : 2 * PAD],
                            jnp.where(which == 2, part[2 * PAD : 3 * PAD], part[3 * PAD :]),
                        ),
                    )
                    state[x + 1, y + 1] = state[x + 1, y + 1] - correction
            j = i - MIX_LAG
            if 0 <= j < steps:
                m = mixed.pop(j)
                residual = [
                    ratio[x, y : y + 1, :] * state[x + 1, y + 1]
                    - scaled[x * 8 + y]
                    - m[:, lane * 128 : (lane + 1) * 128]
                    for lane, (x, y) in enumerate(units[j % count])
                ]
                k = trip * UNROLL + j // count
                moved[j] = jnp.dot(
                    winv[k, :, :192],
                    split3(jnp.concatenate(residual, axis=1)),
                    preferred_element_type=F32,
                )
            if i < steps:
                y_now = [jnp.tanh(state[x + 1, y + 1]) for x, y in units[i % count]]
                mixed[i] = jnp.dot(
                    wmix[:, :192],
                    split3(jnp.concatenate(y_now, axis=1)),
                    preferred_element_type=F32,
                )
        return carry

    lax.fori_loop(0, NMAX // UNROLL, body, 0)


def kernel(
    peers_x, peers_y,
    rate, counts, diffusion, species, mixing, inverses, classes,
    out,
    grid, state, forcing, scaled, ratio, inv_rate, diff, pad, wmix, winv,
    send, recv,
):
    gx, gy = lax.axis_index("gx"), lax.axis_index("gy")
    sides = (
        ("gx", gx, gx > 0, -1),
        ("gx", gx, gx < peers_x - 1, 1),
        ("gy", gy, gy > 0, -1),
        ("gy", gy, gy < peers_y - 1, 1),
    )

    barrier = pltpu.get_barrier_semaphore()
    for axis, index, there, step in sides:
        @pl.when(there)
        def _(axis=axis, index=index, step=step):
            pl.semaphore_signal(barrier, inc=1, device_id={axis: index + step}, device_id_type=MESH)

    def turn_in(x, carry):
        for g in range(7):
            rows = min(8, SPEC - 8 * g)
            block = species[8 * g : 8 * g + rows, x]
            if rows < 8:
                block = jnp.concatenate([block, jnp.zeros((8 - rows, 8, 128), F32)], axis=0)
            grid[x + 1, 1:9, 8 * g : 8 * g + 8, :] = jnp.swapaxes(block, 0, 1)
        return carry

    lax.fori_loop(0, 4, turn_in, 0)

    def halo(buffer, side):
        return (
            buffer.at[0, pl.ds(1, 8)],
            buffer.at[5, pl.ds(1, 8)],
            buffer.at[pl.ds(1, 4), 0],
            buffer.at[pl.ds(1, 4), 9],
        )[side]

    def face(buffer, side):
        return (
            buffer.at[1, pl.ds(1, 8)],
            buffer.at[4, pl.ds(1, 8)],
            buffer.at[pl.ds(1, 4), 1],
            buffer.at[pl.ds(1, 4), 8],
        )[side]

    for side, (axis, index, there, step) in enumerate(sides):
        @pl.when(jnp.logical_not(there))
        def _(side=side):
            for buffer in (grid, state):
                edge = halo(buffer, side)
                edge[...] = jnp.zeros(edge.shape, F32)

    def copy(buffer, round_, side):
        axis, index, there, step = sides[side]
        return pltpu.make_async_remote_copy(
            src_ref=face(buffer, side),
            dst_ref=halo(buffer, side ^ 1),
            send_sem=send.at[round_, side],
            recv_sem=recv.at[round_, side ^ 1],
            device_id={axis: index + step},
            device_id_type=MESH,
        )

    def start(buffer, round_, side):
        @pl.when(sides[side][2])
        def _():
            copy(buffer, round_, side).start()

    def arrived(buffer, round_, side):
        axis, index, there, step = sides[side]

        @pl.when(there)
        def _():
            pltpu.make_async_remote_copy(
                src_ref=face(buffer, side ^ 1),
                dst_ref=halo(buffer, side),
                send_sem=send.at[round_, side ^ 1],
                recv_sem=recv.at[round_, side],
                device_id={axis: index + step},
                device_id_type=MESH,
            ).wait_recv()

    def sent(buffer, round_, side):
        @pl.when(sides[side][2])
        def _():
            copy(buffer, round_, side).wait_send()

    pl.semaphore_wait(barrier, sum(there.astype(jnp.int32) for _, _, there, _ in sides))

    for side in range(4):
        start(grid, 0, side)

    pad[...] = jnp.zeros_like(pad)
    pad[0:SPEC, 0:SPEC] = mixing[...]
    wmix[...] = weight_split(pad[...])
    for c in range(NCLASS):
        pad[0:SPEC, 0:SPEC] = inverses[c] * rate[c]
        w = weight_split(pad[...]).astype(F32)
        for k in range(NMAX):
            winv[k, c * PAD : (c + 1) * PAD, :] = jnp.where(counts[c] > k, w, 0.0).astype(BF16)
    diff[...] = jnp.zeros_like(diff)
    for s in range(SPEC):
        diff[s : s + 1, :] = jnp.full((1, 128), diffusion[s], F32)
    cls = classes[...]
    cell_rate = jnp.where(
        cls == 0, rate[0], jnp.where(cls == 1, rate[1], jnp.where(cls == 2, rate[2], rate[3]))
    )
    inv_rate[...] = 1.0 / cell_rate
    ratio[...] = (1.0 + cell_rate) / cell_rate

    lane = lax.broadcasted_iota(jnp.int32, (PAD, 128), 1)

    def laplace(buffer, x, y):
        here = buffer[x + 1, y + 1]
        total = buffer[x + 2, y + 1] + buffer[x, y + 1]
        total = total + buffer[x + 1, y + 2] + buffer[x + 1, y]
        total = total + jnp.where(lane == 127, 0.0, pltpu.roll(here, 127, 1))
        total = total + jnp.where(lane == 0, 0.0, pltpu.roll(here, 1, 1))
        return total - 6.0 * here, here

    def make_target(x, y):
        lap, here = laplace(grid, x, y)
        force = diff[...] * lap
        target = here + force
        forcing[x * 8 + y] = force
        state[x + 1, y + 1] = target
        scaled[x * 8 + y] = target * inv_rate[x, pl.ds(y, 1), :]

    def over(rows, x0, xstep, fn):
        first, last = rows

        def body(y, carry):
            fn(x0, y)
            fn(x0 + xstep, y)
            return carry

        lax.fori_loop(first, last, body, 0)

    def units_of(xs):
        return [[(x, y), (x, y + 1)] for x in xs for y in range(0, 8, 2)]

    over((1, 7), 1, 1, make_target)
    arrived(grid, 0, 2)
    arrived(grid, 0, 3)
    for y in (0, 7):
        over((y, y + 1), 1, 1, make_target)
    newton(units_of((1, 2)), state, scaled, ratio, classes, wmix, winv)
    arrived(grid, 0, 0)
    arrived(grid, 0, 1)
    over((0, 8), 0, 3, make_target)
    newton(units_of((0, 3)), state, scaled, ratio, classes, wmix, winv)
    for side in range(4):
        start(state, 1, side)

    def finish(x, y):
        lap, here = laplace(state, x, y)
        forcing[x * 8 + y] = here + 0.5 * (diff[...] * lap - forcing[x * 8 + y])

    def turn_out(x):
        for g in range(7):
            rows = min(8, SPEC - 8 * g)
            block = jnp.swapaxes(forcing[x * 8 : x * 8 + 8, 8 * g : 8 * g + 8, :], 0, 1)
            out[8 * g : 8 * g + rows, x] = block[0:rows]

    over((1, 7), 1, 1, finish)
    arrived(state, 1, 2)
    arrived(state, 1, 3)
    for y in (0, 7):
        over((y, y + 1), 1, 1, finish)
    turn_out(1)
    turn_out(2)
    arrived(state, 1, 0)
    arrived(state, 1, 1)
    over((0, 8), 0, 3, finish)
    turn_out(0)
    turn_out(3)
    for round_, buffer in ((0, grid), (1, state)):
        for side in range(4):
            sent(buffer, round_, side)


def solution(mesh):
    peers_x, peers_y = mesh.shape["gx"], mesh.shape["gy"]

    def local(species, diffusion, class_rate, mixing, inverses, newton_counts, cell_class):
        vmem = pl.BlockSpec(memory_space=pltpu.VMEM)
        smem = pl.BlockSpec(memory_space=pltpu.SMEM)
        return pl.pallas_call(
            functools.partial(kernel, peers_x, peers_y),
            out_shape=jax.ShapeDtypeStruct(species.shape, F32),
            in_specs=[smem, smem, smem, vmem, vmem, vmem, vmem],
            out_specs=vmem,
            scratch_shapes=[
                pltpu.VMEM((6, 10, PAD, 128), F32),
                pltpu.VMEM((6, 10, PAD, 128), F32),
                pltpu.VMEM((32, PAD, 128), F32),
                pltpu.VMEM((32, PAD, 128), F32),
                pltpu.VMEM((4, 8, 128), F32),
                pltpu.VMEM((4, 8, 128), F32),
                pltpu.VMEM((PAD, 128), F32),
                pltpu.VMEM((PAD, 128), F32),
                pltpu.VMEM((PAD, 256), BF16),
                pltpu.VMEM((NMAX, NCLASS * PAD, 256), BF16),
                pltpu.SemaphoreType.DMA((2, 4)),
                pltpu.SemaphoreType.DMA((2, 4)),
            ],
            compiler_params=pltpu.CompilerParams(
                collective_id=0, has_side_effects=True, vmem_limit_bytes=48 * 1024 * 1024
            ),
            name="section",
        )(class_rate, newton_counts, diffusion, species, mixing, inverses, cell_class)

    in_specs = (P(None, "gx", "gy", None), P(), P(), P(), P(), P(), P("gx", "gy", None))
    out_specs = P(None, "gx", "gy", None)
    return jax.shard_map(local, mesh=mesh, in_specs=in_specs, out_specs=out_specs, check_vma=False)
```

```python
import functools

import jax
import jax.numpy as jnp
from jax import lax
from jax.experimental import pallas as pl
from jax.experimental.pallas import tpu as pltpu
from jax.sharding import PartitionSpec as P

SPEC = 53
PAD = 56
NCLASS = 4
NMAX = 8
F32, BF16 = jnp.float32, jnp.bfloat16
MESH = pl.DeviceIdType.MESH

LAG = 4


def parts_of(v):
    v = jnp.concatenate([v, jnp.zeros((8, v.shape[1]), F32)], axis=0)
    high = v.astype(BF16)
    return high, (v - high.astype(F32)).astype(BF16)


def halves_of(w):
    high = w.astype(BF16).astype(F32)
    return high, w - high


def pick(out, which):
    return jnp.where(
        which == 0,
        out[0:PAD],
        jnp.where(
            which == 1,
            out[PAD : 2 * PAD],
            jnp.where(which == 2, out[2 * PAD : 3 * PAD], out[3 * PAD :]),
        ),
    )


def newton(units, state, drift, cell_count, classes, wstep, wdrift):
    def finish_unit(unit, out, fn):
        for lane, (x, y) in enumerate(unit):
            which = jnp.broadcast_to(classes[x, y : y + 1, :], (PAD, 128))
            fn(x, y, pick(out[:, lane * 128 : (lane + 1) * 128], which))

    def values(unit):
        return jnp.concatenate([state[x + 1, y + 1] for x, y in unit], axis=1)

    def set_drift(x, y, value):
        drift[x * 8 + y] = value

    for unit in units:
        high, low = parts_of(values(unit))
        rhs = jnp.concatenate([high, low, high], axis=0)
        finish_unit(unit, jnp.dot(wdrift[:, :192], rhs, preferred_element_type=F32), set_drift)

    count = len(units)
    steps = count * NMAX
    moved = {}
    for i in range(steps + LAG):
        j = i - LAG
        if 0 <= j < steps:

            def move(x, y, value, k=j // count):
                active = jnp.broadcast_to(cell_count[x, y : y + 1, :] > k, (PAD, 128))
                change = jnp.where(active, value + drift[x * 8 + y], 0.0)
                state[x + 1, y + 1] = state[x + 1, y + 1] + change

            finish_unit(units[j % count], moved.pop(j), move)
        if i < steps:
            now = values(units[i % count])
            t_high, t_low = parts_of(jnp.tanh(now))
            y_high, y_low = parts_of(now)
            rhs = jnp.concatenate([t_high, t_low, y_high, y_low, t_high, y_high], axis=0)
            moved[i] = jnp.dot(wstep[...], rhs, preferred_element_type=F32)


def kernel(
    peers_x, peers_y,
    rate_in, counts_in, diffusion_in, species_in, mixing_in, inverses_in, classes_in,
    out,
    species, mixing, inverses, classes, rate, counts, diffusion,
    grid, state, forcing, drift, cell_count, diff, mix_pad, inv_pad, wstep, wdrift,
    loaded, send, recv,
):
    gx, gy = lax.axis_index("gx"), lax.axis_index("gy")
    sides = (
        ("gx", gx, gx > 0, -1),
        ("gx", gx, gx < peers_x - 1, 1),
        ("gy", gy, gy > 0, -1),
        ("gy", gy, gy < peers_y - 1, 1),
    )

    barrier = pltpu.get_barrier_semaphore()
    for axis, index, there, step in sides:
        @pl.when(there)
        def _(axis=axis, index=index, step=step):
            pl.semaphore_signal(barrier, inc=1, device_id={axis: index + step}, device_id_type=MESH)

    loads = [
        pltpu.make_async_copy(species_in.at[:, x], species.at[:, x], loaded.at[x]) for x in range(4)
    ] + [
        pltpu.make_async_copy(src, dst, loaded.at[4 + i])
        for i, (src, dst) in enumerate((
            (mixing_in, mixing), (inverses_in, inverses), (classes_in, classes),
            (rate_in, rate), (counts_in, counts), (diffusion_in, diffusion),
        ))
    ]
    for i in (0, 3, 1, 2, 4, 5, 6, 7, 8, 9):
        loads[i].start()

    def halo(buffer, side, part):
        return (
            buffer.at[0, pl.ds(1 + 4 * part, 4)],
            buffer.at[5, pl.ds(1 + 4 * part, 4)],
            buffer.at[pl.ds(1, 4), 0],
            buffer.at[pl.ds(1, 4), 9],
        )[side]

    def face(buffer, side, part):
        return (
            buffer.at[1, pl.ds(1 + 4 * part, 4)],
            buffer.at[4, pl.ds(1 + 4 * part, 4)],
            buffer.at[pl.ds(1, 4), 1],
            buffer.at[pl.ds(1, 4), 8],
        )[side]

    parts = (2, 2, 1, 1)
    for side in range(4):
        @pl.when(jnp.logical_not(sides[side][2]))
        def _(side=side):
            for buffer in (grid, state):
                for part in range(parts[side]):
                    edge = halo(buffer, side, part)
                    edge[...] = jnp.zeros(edge.shape, F32)

    def copy(buffer, round_, side, part):
        axis, index, there, step = sides[side]
        return pltpu.make_async_remote_copy(
            src_ref=face(buffer, side, part),
            dst_ref=halo(buffer, side ^ 1, part),
            send_sem=send.at[round_, side, part],
            recv_sem=recv.at[round_, side ^ 1, part],
            device_id={axis: index + step},
            device_id_type=MESH,
        )

    def start(buffer, round_, side, part=0):
        @pl.when(sides[side][2])
        def _():
            copy(buffer, round_, side, part).start()

    def arrived(buffer, round_, side, part=0):
        axis, index, there, step = sides[side]

        @pl.when(there)
        def _():
            pltpu.make_async_remote_copy(
                src_ref=face(buffer, side ^ 1, part),
                dst_ref=halo(buffer, side, part),
                send_sem=send.at[round_, side ^ 1, part],
                recv_sem=recv.at[round_, side, part],
                device_id={axis: index + step},
                device_id_type=MESH,
            ).wait_recv()

    def sent(buffer, round_, side, part=0):
        @pl.when(sides[side][2])
        def _():
            copy(buffer, round_, side, part).wait_send()

    def turn_in(x):
        loads[x].wait()
        for g in range(7):
            rows = min(8, SPEC - 8 * g)
            block = species[8 * g : 8 * g + rows, x]
            if rows < 8:
                block = jnp.concatenate([block, jnp.zeros((8 - rows, 8, 128), F32)], axis=0)
            grid[x + 1, 1:9, 8 * g : 8 * g + 8, :] = jnp.swapaxes(block, 0, 1)

    turn_in(0)
    turn_in(3)
    pl.semaphore_wait(barrier, sum(there.astype(jnp.int32) for _, _, there, _ in sides))
    for side in (0, 1):
        start(grid, 0, side, 0)
    for side in (0, 1):
        start(grid, 0, side, 1)
    turn_in(1)
    turn_in(2)
    for side in (2, 3):
        start(grid, 0, side)
    for i in range(4, 10):
        loads[i].wait()

    mix_pad[...] = jnp.zeros_like(mix_pad)
    mix_pad[0:SPEC, 0:SPEC] = mixing[...]
    inv_pad[...] = jnp.zeros_like(inv_pad)
    for c in range(NCLASS):
        inv_pad[c * PAD : c * PAD + SPEC, 0:SPEC] = inverses[:, c, :]
    product = jnp.dot(
        inv_pad[...], mix_pad[...], precision=lax.Precision.HIGHEST, preferred_element_type=F32
    )
    for c in range(NCLASS):
        rows = slice(c * PAD, (c + 1) * PAD)
        i_high, i_low = halves_of(inv_pad[rows])
        p_high, p_low = halves_of(rate[c] * product[rows])
        q_high, q_low = halves_of((-1.0 - rate[c]) * inv_pad[rows])
        wdrift[rows, 0:128] = (i_high + pltpu.roll(i_high, 64, 1)).astype(BF16)
        wdrift[rows, 128:256] = i_low.astype(BF16)
        wstep[rows, 0:128] = (p_high + pltpu.roll(p_high, 64, 1)).astype(BF16)
        wstep[rows, 128:256] = (q_high + pltpu.roll(q_high, 64, 1)).astype(BF16)
        wstep[rows, 256:384] = (p_low + pltpu.roll(q_low, 64, 1)).astype(BF16)
    diff[...] = jnp.zeros_like(diff)
    for s in range(SPEC):
        diff[s : s + 1, :] = jnp.full((1, 128), diffusion[s], F32)
    cls = classes[...]
    cell_count[...] = jnp.where(
        cls == 0, counts[0], jnp.where(cls == 1, counts[1], jnp.where(cls == 2, counts[2], counts[3]))
    )

    lane = lax.broadcasted_iota(jnp.int32, (PAD, 128), 1)

    def laplace(buffer, x, y):
        here = buffer[x + 1, y + 1]
        total = buffer[x + 2, y + 1] + buffer[x, y + 1]
        total = total + buffer[x + 1, y + 2] + buffer[x + 1, y]
        total = total + jnp.where(lane == 127, 0.0, pltpu.roll(here, 127, 1))
        total = total + jnp.where(lane == 0, 0.0, pltpu.roll(here, 1, 1))
        return total - 6.0 * here, here

    def make_target(x, y):
        lap, here = laplace(grid, x, y)
        force = diff[...] * lap
        target = here + force
        forcing[x * 8 + y] = force
        state[x + 1, y + 1] = target

    def finish(x, y):
        lap, here = laplace(state, x, y)
        forcing[x * 8 + y] = here + 0.5 * (diff[...] * lap - forcing[x * 8 + y])

    def turn_out(x):
        for g in range(7):
            rows = min(8, SPEC - 8 * g)
            block = jnp.swapaxes(forcing[x * 8 : x * 8 + 8, 8 * g : 8 * g + 8, :], 0, 1)
            out[8 * g : 8 * g + rows, x] = block[0:rows]

    def over(first, last, xs, fn):
        for y in range(first, last):
            for x in xs:
                fn(x, y)

    def solve(xs, ys):
        units = [[(x, y), (x, y + 1)] for y in ys for x in xs]
        newton(units, state, drift, cell_count, classes, wstep, wdrift)

    def solve_edge_rows():
        over(0, 2, (1, 2), make_target)
        over(6, 8, (1, 2), make_target)
        solve((1, 2), (0, 6))

    over(2, 6, (1, 2), make_target)
    solve((1, 2), (2, 4))
    for side in (2, 3):
        arrived(grid, 0, side)
    last = lax.rem(gx, 8) == 7
    pl.when(jnp.logical_not(last))(solve_edge_rows)
    for part in range(2):
        for side in (1, 0):
            arrived(grid, 0, side, part)
        over(4 * part, 4 * part + 4, (0, 3), make_target)
        solve((0, 3), (4 * part, 4 * part + 2))
        for side in (1, 0):
            start(state, 1, side, part)
    pl.when(last)(solve_edge_rows)
    for side in (2, 3):
        start(state, 1, side)

    over(1, 7, (1, 2), finish)
    for side in (2, 3):
        arrived(state, 1, side)
    over(0, 1, (1, 2), finish)
    over(7, 8, (1, 2), finish)
    turn_out(1)
    turn_out(2)
    for x, side in ((3, 1), (0, 0)):
        for part in range(2):
            arrived(state, 1, side, part)
            over(4 * part, 4 * part + 4, (x,), finish)
        turn_out(x)
    for round_, buffer in ((0, grid), (1, state)):
        for side in range(4):
            for part in range(parts[side]):
                sent(buffer, round_, side, part)


def solution(mesh):
    peers_x, peers_y = mesh.shape["gx"], mesh.shape["gy"]

    def local(species, diffusion, class_rate, mixing, inverses, newton_counts, cell_class):
        hbm = pl.BlockSpec(memory_space=pltpu.HBM)
        operands = (
            class_rate, newton_counts, diffusion, species, mixing,
            jnp.transpose(inverses, (1, 0, 2)), cell_class,
        )
        return pl.pallas_call(
            functools.partial(kernel, peers_x, peers_y),
            out_shape=jax.ShapeDtypeStruct(species.shape, F32),
            in_specs=[hbm] * 7,
            out_specs=pl.BlockSpec(memory_space=pltpu.VMEM),
            scratch_shapes=[
                pltpu.VMEM((SPEC, 4, 8, 128), F32),
                pltpu.VMEM((SPEC, SPEC), F32),
                pltpu.VMEM((SPEC, NCLASS, SPEC), F32),
                pltpu.VMEM((4, 8, 128), jnp.int32),
                pltpu.SMEM((NCLASS,), F32),
                pltpu.SMEM((NCLASS,), jnp.int32),
                pltpu.SMEM((SPEC,), F32),
                pltpu.VMEM((6, 10, PAD, 128), F32),
                pltpu.VMEM((6, 10, PAD, 128), F32),
                pltpu.VMEM((32, PAD, 128), F32),
                pltpu.VMEM((32, PAD, 128), F32),
                pltpu.VMEM((4, 8, 128), jnp.int32),
                pltpu.VMEM((PAD, 128), F32),
                pltpu.VMEM((128, 128), F32),
                pltpu.VMEM((NCLASS * PAD, 128), F32),
                pltpu.VMEM((NCLASS * PAD, 384), BF16),
                pltpu.VMEM((NCLASS * PAD, 256), BF16),
                pltpu.SemaphoreType.DMA((10,)),
                pltpu.SemaphoreType.DMA((2, 4, 2)),
                pltpu.SemaphoreType.DMA((2, 4, 2)),
            ],
            compiler_params=pltpu.CompilerParams(
                collective_id=0, has_side_effects=True, vmem_limit_bytes=48 * 1024 * 1024
            ),
            name="section",
        )(*(pltpu.with_memory_space_constraint(v, pltpu.HBM) for v in operands))

    in_specs = (P(None, "gx", "gy", None), P(), P(), P(), P(), P(), P("gx", "gy", None))
    out_specs = P(None, "gx", "gy", None)
    return jax.shard_map(local, mesh=mesh, in_specs=in_specs, out_specs=out_specs, check_vma=False)
```

```python
import functools

import jax
import jax.numpy as jnp
from jax import lax
from jax.experimental import pallas as pl
from jax.experimental.pallas import tpu as pltpu
from jax.sharding import PartitionSpec as P

SPEC = 53
PAD = 56
NCLASS = 4
NMAX = 8
F32, BF16 = jnp.float32, jnp.bfloat16
MESH = pl.DeviceIdType.MESH

LAG = 4


def parts_of(v):
    v = jnp.concatenate([v, jnp.zeros((8, v.shape[1]), F32)], axis=0)
    high = v.astype(BF16)
    return high, (v - high.astype(F32)).astype(BF16)


def halves_of(w):
    high = w.astype(BF16).astype(F32)
    return high, w - high


def pick(out, which):
    return jnp.where(
        which == 0,
        out[0:PAD],
        jnp.where(
            which == 1,
            out[PAD : 2 * PAD],
            jnp.where(which == 2, out[2 * PAD : 3 * PAD], out[3 * PAD :]),
        ),
    )


def newton(units, state, drift, cell_count, classes, wstep, wdrift):
    def finish_unit(unit, out, fn):
        for lane, (x, y) in enumerate(unit):
            which = jnp.broadcast_to(classes[x, y : y + 1, :], (PAD, 128))
            fn(x, y, pick(out[:, lane * 128 : (lane + 1) * 128], which))

    def values(unit):
        return jnp.concatenate([state[x + 1, y + 1] for x, y in unit], axis=1)

    def set_drift(x, y, value):
        drift[x * 8 + y] = value

    for unit in units:
        high, low = parts_of(values(unit))
        rhs = jnp.concatenate([high, low, high], axis=0)
        finish_unit(unit, jnp.dot(wdrift[:, :192], rhs, preferred_element_type=F32), set_drift)

    count = len(units)
    steps = count * NMAX
    moved = {}
    for i in range(steps + LAG):
        j = i - LAG
        if 0 <= j < steps:

            def move(x, y, value, k=j // count):
                active = jnp.broadcast_to(cell_count[x, y : y + 1, :] > k, (PAD, 128))
                change = jnp.where(active, value + drift[x * 8 + y], 0.0)
                state[x + 1, y + 1] = state[x + 1, y + 1] + change

            finish_unit(units[j % count], moved.pop(j), move)
        if i < steps:
            now = values(units[i % count])
            t_high, t_low = parts_of(jnp.tanh(now))
            y_high, y_low = parts_of(now)
            rhs = jnp.concatenate([t_high, t_low, y_high, y_low, t_high, y_high], axis=0)
            moved[i] = jnp.dot(wstep[...], rhs, preferred_element_type=F32)


def kernel(
    peers_x, peers_y,
    rate_in, counts_in, diffusion_in, species_in, mixing_in, inverses_in, classes_in,
    out,
    species, mixing, inverses, classes, rate, counts, diffusion,
    grid, state, forcing, drift, cell_count, diff, mix_pad, inv_pad, wstep, wdrift,
    loaded, send, recv,
):
    gx, gy = lax.axis_index("gx"), lax.axis_index("gy")
    sides = (
        ("gx", gx, gx > 0, -1),
        ("gx", gx, gx < peers_x - 1, 1),
        ("gy", gy, gy > 0, -1),
        ("gy", gy, gy < peers_y - 1, 1),
    )

    for x in (0, 5):
        grid[x, 1:9, SPEC:PAD, :] = jnp.zeros((8, PAD - SPEC, 128), F32)
        state[x, 1:9, SPEC:PAD, :] = jnp.zeros((8, PAD - SPEC, 128), F32)
    barrier = pltpu.get_barrier_semaphore()
    for axis, index, there, step in sides:
        @pl.when(there)
        def _(axis=axis, index=index, step=step):
            pl.semaphore_signal(barrier, inc=1, device_id={axis: index + step}, device_id_type=MESH)

    loads = [
        pltpu.make_async_copy(species_in.at[:, x], species.at[:, x], loaded.at[x]) for x in range(4)
    ] + [
        pltpu.make_async_copy(src, dst, loaded.at[4 + i])
        for i, (src, dst) in enumerate((
            (mixing_in, mixing), (inverses_in, inverses), (classes_in, classes),
            (rate_in, rate), (counts_in, counts), (diffusion_in, diffusion),
        ))
    ]
    for i in (0, 3, 1, 2, 4, 5, 6, 7, 8, 9):
        loads[i].start()

    def halo(buffer, side, part):
        return (
            buffer.at[0, pl.ds(1 + 4 * part, 4), pl.ds(0, SPEC)],
            buffer.at[5, pl.ds(1 + 4 * part, 4), pl.ds(0, SPEC)],
            buffer.at[pl.ds(1, 4), 0],
            buffer.at[pl.ds(1, 4), 9],
        )[side]

    def face(buffer, side, part):
        return (
            buffer.at[1, pl.ds(1 + 4 * part, 4), pl.ds(0, SPEC)],
            buffer.at[4, pl.ds(1 + 4 * part, 4), pl.ds(0, SPEC)],
            buffer.at[pl.ds(1, 4), 1],
            buffer.at[pl.ds(1, 4), 8],
        )[side]

    parts = (2, 2, 1, 1)
    for side in range(4):
        @pl.when(jnp.logical_not(sides[side][2]))
        def _(side=side):
            for buffer in (grid, state):
                for part in range(parts[side]):
                    edge = halo(buffer, side, part)
                    edge[...] = jnp.zeros(edge.shape, F32)

    def copy(buffer, round_, side, part):
        axis, index, there, step = sides[side]
        return pltpu.make_async_remote_copy(
            src_ref=face(buffer, side, part),
            dst_ref=halo(buffer, side ^ 1, part),
            send_sem=send.at[round_, side, part],
            recv_sem=recv.at[round_, side ^ 1, part],
            device_id={axis: index + step},
            device_id_type=MESH,
        )

    def start(buffer, round_, side, part=0):
        @pl.when(sides[side][2])
        def _():
            copy(buffer, round_, side, part).start()

    def arrived(buffer, round_, side, part=0):
        axis, index, there, step = sides[side]

        @pl.when(there)
        def _():
            pltpu.make_async_remote_copy(
                src_ref=face(buffer, side ^ 1, part),
                dst_ref=halo(buffer, side, part),
                send_sem=send.at[round_, side ^ 1, part],
                recv_sem=recv.at[round_, side, part],
                device_id={axis: index + step},
                device_id_type=MESH,
            ).wait_recv()

    def sent(buffer, round_, side, part=0):
        @pl.when(sides[side][2])
        def _():
            copy(buffer, round_, side, part).wait_send()

    def turn_in(x):
        loads[x].wait()
        for g in range(7):
            rows = min(8, SPEC - 8 * g)
            block = species[8 * g : 8 * g + rows, x]
            if rows < 8:
                block = jnp.concatenate([block, jnp.zeros((8 - rows, 8, 128), F32)], axis=0)
            grid[x + 1, 1:9, 8 * g : 8 * g + 8, :] = jnp.swapaxes(block, 0, 1)

    turn_in(0)
    turn_in(3)
    pl.semaphore_wait(barrier, sum(there.astype(jnp.int32) for _, _, there, _ in sides))
    for side in (0, 1):
        start(grid, 0, side, 0)
    for side in (0, 1):
        start(grid, 0, side, 1)
    turn_in(1)
    turn_in(2)
    for side in (2, 3):
        start(grid, 0, side)
    for i in range(4, 10):
        loads[i].wait()

    mix_pad[...] = jnp.zeros_like(mix_pad)
    mix_pad[0:SPEC, 0:SPEC] = mixing[...]
    inv_pad[...] = jnp.zeros_like(inv_pad)
    for c in range(NCLASS):
        inv_pad[c * PAD : c * PAD + SPEC, 0:SPEC] = inverses[:, c, :]
    product = jnp.dot(
        inv_pad[...], mix_pad[...], precision=lax.Precision.HIGHEST, preferred_element_type=F32
    )
    for c in range(NCLASS):
        rows = slice(c * PAD, (c + 1) * PAD)
        i_high, i_low = halves_of(inv_pad[rows])
        p_high, p_low = halves_of(rate[c] * product[rows])
        q_high, q_low = halves_of((-1.0 - rate[c]) * inv_pad[rows])
        wdrift[rows, 0:128] = (i_high + pltpu.roll(i_high, 64, 1)).astype(BF16)
        wdrift[rows, 128:256] = i_low.astype(BF16)
        wstep[rows, 0:128] = (p_high + pltpu.roll(p_high, 64, 1)).astype(BF16)
        wstep[rows, 128:256] = (q_high + pltpu.roll(q_high, 64, 1)).astype(BF16)
        wstep[rows, 256:384] = (p_low + pltpu.roll(q_low, 64, 1)).astype(BF16)
    diff[...] = jnp.zeros_like(diff)
    for s in range(SPEC):
        diff[s : s + 1, :] = jnp.full((1, 128), diffusion[s], F32)
    cls = classes[...]
    cell_count[...] = jnp.where(
        cls == 0, counts[0], jnp.where(cls == 1, counts[1], jnp.where(cls == 2, counts[2], counts[3]))
    )

    lane = lax.broadcasted_iota(jnp.int32, (PAD, 128), 1)

    def laplace(buffer, x, y):
        here = buffer[x + 1, y + 1]
        total = buffer[x + 2, y + 1] + buffer[x, y + 1]
        total = total + buffer[x + 1, y + 2] + buffer[x + 1, y]
        total = total + jnp.where(lane == 127, 0.0, pltpu.roll(here, 127, 1))
        total = total + jnp.where(lane == 0, 0.0, pltpu.roll(here, 1, 1))
        return total - 6.0 * here, here

    def make_target(x, y):
        lap, here = laplace(grid, x, y)
        force = diff[...] * lap
        target = here + force
        forcing[x * 8 + y] = force
        state[x + 1, y + 1] = target

    def finish(x, y):
        lap, here = laplace(state, x, y)
        forcing[x * 8 + y] = here + 0.5 * (diff[...] * lap - forcing[x * 8 + y])

    def turn_out(x):
        for g in range(7):
            rows = min(8, SPEC - 8 * g)
            block = jnp.swapaxes(forcing[x * 8 : x * 8 + 8, 8 * g : 8 * g + 8, :], 0, 1)
            out[8 * g : 8 * g + rows, x] = block[0:rows]

    def over(first, last, xs, fn):
        for y in range(first, last):
            for x in xs:
                fn(x, y)

    def solve(xs, ys):
        units = [[(x, y), (x, y + 1)] for y in ys for x in xs]
        newton(units, state, drift, cell_count, classes, wstep, wdrift)

    def solve_edge_rows():
        over(0, 2, (1, 2), make_target)
        over(6, 8, (1, 2), make_target)
        solve((1, 2), (0, 6))

    over(2, 6, (1, 2), make_target)
    solve((1, 2), (2, 4))
    for side in (2, 3):
        arrived(grid, 0, side)
    last = lax.rem(gx, 8) == 7
    pl.when(jnp.logical_not(last))(solve_edge_rows)
    for part in range(2):
        for side in (1, 0):
            arrived(grid, 0, side, part)
        over(4 * part, 4 * part + 4, (0, 3), make_target)
        solve((0, 3), (4 * part, 4 * part + 2))
        for side in (1, 0):
            start(state, 1, side, part)
    pl.when(last)(solve_edge_rows)
    for side in (2, 3):
        start(state, 1, side)

    over(1, 7, (1, 2), finish)
    for side in (2, 3):
        arrived(state, 1, side)
    over(0, 1, (1, 2), finish)
    over(7, 8, (1, 2), finish)
    turn_out(1)
    turn_out(2)
    for x, side in ((3, 1), (0, 0)):
        for part in range(2):
            arrived(state, 1, side, part)
            over(4 * part, 4 * part + 4, (x,), finish)
        turn_out(x)
    for round_, buffer in ((0, grid), (1, state)):
        for side in range(4):
            for part in range(parts[side]):
                sent(buffer, round_, side, part)


def solution(mesh):
    peers_x, peers_y = mesh.shape["gx"], mesh.shape["gy"]

    def local(species, diffusion, class_rate, mixing, inverses, newton_counts, cell_class):
        hbm = pl.BlockSpec(memory_space=pltpu.HBM)
        operands = (
            class_rate, newton_counts, diffusion, species, mixing,
            jnp.transpose(inverses, (1, 0, 2)), cell_class,
        )
        return pl.pallas_call(
            functools.partial(kernel, peers_x, peers_y),
            out_shape=jax.ShapeDtypeStruct(species.shape, F32),
            in_specs=[hbm] * 7,
            out_specs=pl.BlockSpec(memory_space=pltpu.VMEM),
            scratch_shapes=[
                pltpu.VMEM((SPEC, 4, 8, 128), F32),
                pltpu.VMEM((SPEC, SPEC), F32),
                pltpu.VMEM((SPEC, NCLASS, SPEC), F32),
                pltpu.VMEM((4, 8, 128), jnp.int32),
                pltpu.SMEM((NCLASS,), F32),
                pltpu.SMEM((NCLASS,), jnp.int32),
                pltpu.SMEM((SPEC,), F32),
                pltpu.VMEM((6, 10, PAD, 128), F32),
                pltpu.VMEM((6, 10, PAD, 128), F32),
                pltpu.VMEM((32, PAD, 128), F32),
                pltpu.VMEM((32, PAD, 128), F32),
                pltpu.VMEM((4, 8, 128), jnp.int32),
                pltpu.VMEM((PAD, 128), F32),
                pltpu.VMEM((128, 128), F32),
                pltpu.VMEM((NCLASS * PAD, 128), F32),
                pltpu.VMEM((NCLASS * PAD, 384), BF16),
                pltpu.VMEM((NCLASS * PAD, 256), BF16),
                pltpu.SemaphoreType.DMA((10,)),
                pltpu.SemaphoreType.DMA((2, 4, 2)),
                pltpu.SemaphoreType.DMA((2, 4, 2)),
            ],
            compiler_params=pltpu.CompilerParams(
                collective_id=0, has_side_effects=True, vmem_limit_bytes=48 * 1024 * 1024
            ),
            name="section",
        )(*(pltpu.with_memory_space_constraint(v, pltpu.HBM) for v in operands))

    in_specs = (P(None, "gx", "gy", None), P(), P(), P(), P(), P(), P("gx", "gy", None))
    out_specs = P(None, "gx", "gy", None)
    return jax.shard_map(local, mesh=mesh, in_specs=in_specs, out_specs=out_specs, check_vma=False)
```
